32 devices in a mesh: grp: 2 (over y), col: 4 (over z), row: 2 (over x), dir: 2 (over core).
Axes of the slice: x: 2, y: 2, z: 4, core: 2. Of those that a mesh axis runs over, the one named last changes fastest.
Arguments:
- slopes_in: bfloat16 [512, 8192], P(None, ('grp', 'col')), parts along dimension 1, may hold values from -6 to 6
- basis_left: bfloat16 [12, 16, 256, 256], P(('row', 'dir'), 'col'), may hold values from -0.09375 to 0.09375
- basis_right: bfloat16 [12, 16, 256, 256], P(('row', 'dir'), 'col'), may hold values from -0.375 to 0.375
- rank_blocks: int32 [12, 16], P(('row', 'dir'), 'col'), may hold values from 1 to 4
- tile_owner: int32 [16], replicated, may hold values from 0 to 15, each once
- footprint: int32 [4, 4, 4, 2048], P(('row', 'dir')), may hold values from 0 to 767
- trace_weight: float32 [4, 4, 4, 2048], P(('row', 'dir')), may hold values from 0 to 0.5
- fitting: bfloat16 [2048, 4096], P(None, 'col'), may hold values from -0.125 to 0.125
Outputs:
- commands: bfloat16 [4, 1024, 4096], P(('row', 'dir'), 'grp', 'col'), parts along dimension 1
The draws below stay inside these ranges and needn't reach their ends.
There are 2 independent parts, one for each index of `grp`. The reference program is written for one: setup_inputs(seed, part) draws one part's arguments, and reference() takes and returns one part's arrays. A program takes and returns all parts, laid end to end along the dimension named above; an argument that names none is the same for every part. Nothing has to cross between parts.
Inputs may be any that keep to these rules, and one draw needn't show every extreme that they name: rank_blocks[i, k] is the number of leading blocks of 64 columns of tile (i, k) that are live. `tile_owner`: each slope block appears in exactly one tile slot. `footprint`: indices into one layer's points.
All inputs are finite; a program needn't handle non-finite values.
Results may differ from the reference program's by a relative error of at most 0.0064.
Values may be sent and summed in bfloat16 or wider, within the bound.
No kernel may reach another device: no remote copies, remote signals or barrier semaphores. Data moves between devices by JAX's collectives and lax.ppermute only.
A program may use at most 128 MiB of HBM per device.

```python
import jax
import jax.numpy as jnp
from jax import lax

NB = 256
RB = 64
RMAX = 4
F = 512
L = 4
M = 2048
ACT = 4096
RK = 256
TR = 12
TC = 16
P_SIZE = 3072
S = 4096
G = 768
ND = 4


def touch_ends(drawn, stream_key, smallest, top_value):
    spot = [jax.random.randint(jax.random.fold_in(stream_key, axis), (), 0, length) for axis, length in enumerate(drawn.shape)]
    main_axis = drawn.shape.index(max(drawn.shape))
    neighbour = spot[:main_axis] + [(spot[main_axis] + 1) % drawn.shape[main_axis]] + spot[main_axis + 1:]
    return drawn.at[tuple(spot)].set(smallest).at[tuple(neighbour)].set(top_value)


def block_levels(own_key, dims, cuts, least, top_value):
    def one(position, parts):
        heights = jax.random.uniform(jax.random.fold_in(jax.random.fold_in(own_key, 6), position), (parts,), jnp.float32, least / len(cuts), top_value / len(cuts))
        return jnp.repeat(jnp.exp(heights), dims[position] // parts).reshape((-1,) + (1,) * (len(dims) - position - 1))

    level = one(*cuts[0])
    for cut in cuts[1:]:
        level = level * one(*cut)
    return level


def centred(rng, extent, spread, limit, split=(), held_as=jnp.bfloat16):
    entries = jax.random.normal(rng, extent, jnp.float32) * spread
    if len(split) > 0:
        entries = block_levels(rng, extent, split, -0.22, 0.18) * entries
    return jnp.clip(entries, min=-limit, max=limit).astype(held_as)


def setup_inputs(seed: int = 0, part: int = 0) -> dict:
    arg_keys = jax.random.split(jax.random.key(seed), 9)
    part_keys = jax.random.split(jax.random.fold_in(arg_keys[8], part), 9)
    return {
        "slopes_in": centred(part_keys[0], (F, S), 1.0, 6.0, ((1, 4),)),
        "basis_left": centred(arg_keys[1], (TR, TC, NB, RK), (RK * TC) ** -0.5, 0.09375, ((0, 4), (1, 4))),
        "basis_right": centred(arg_keys[2], (TR, TC, NB, RK), NB ** -0.5, 0.375, ((0, 4), (1, 4))),
        "rank_blocks": touch_ends(jax.random.randint(arg_keys[3], (TR, TC), 1, RMAX + 1), jax.random.fold_in(arg_keys[3], 1), 1, RMAX).astype(jnp.int32),
        "tile_owner": jax.random.permutation(arg_keys[4], TC).astype(jnp.int32),
        "footprint": touch_ends(jax.random.randint(arg_keys[5], (ND, L, 4, M), 0, G), jax.random.fold_in(arg_keys[5], 1), 0, G - 1).astype(jnp.int32),
        "trace_weight": jnp.clip(0.5 * jax.random.uniform(arg_keys[6], (ND, L, 4, M), jnp.float32) ** block_levels(arg_keys[6], (ND, L, 4, M), ((0, 4),), -0.2, 0.2), 0.0, 0.5),
        "fitting": centred(arg_keys[7], (M, ACT), M ** -0.5, 0.125, ((1, 4),)),
    }


def reference(slopes_in, basis_left, basis_right, rank_blocks, tile_owner, footprint, trace_weight, fitting):
    blocks = slopes_in.reshape(F, TC, NB)
    chosen = jnp.take(blocks, tile_owner.astype(jnp.int32), axis=1)
    chosen_f = chosen.astype(jnp.float32)
    columns = jnp.arange(RK, dtype=jnp.int32) // RB

    def one_row(packed):
        left, right, ranks = packed
        coeffs = jnp.einsum('fkn,knr->kfr', chosen_f, right.astype(jnp.float32))
        live = columns[None, None, :] < ranks[:, None, None]
        coeffs = jnp.where(live, coeffs, 0.0).astype(jnp.bfloat16)
        return jnp.einsum('kfr,knr->fn', coeffs.astype(jnp.float32), left.astype(jnp.float32))

    rows = lax.map(one_row, (basis_left, basis_right, rank_blocks))
    layers = jnp.transpose(rows, (1, 0, 2)).reshape(F, P_SIZE).astype(jnp.bfloat16)
    shifts = (jnp.arange(L, dtype=jnp.int32) * G)[:, None, None]

    def one_direction(packed):
        points, weights = packed
        flat = (points + shifts).reshape(-1)
        values = jnp.take(layers, flat, axis=1).astype(jnp.float32).reshape(F, L, 4, M)
        pupil = jnp.sum(values * weights[None], axis=(1, 2)).astype(jnp.bfloat16)
        return jnp.dot(pupil, fitting, preferred_element_type=jnp.float32).astype(jnp.bfloat16)

    return lax.map(one_direction, (footprint, trace_weight))
```

```python
import jax
import jax.numpy as jnp
from jax import lax
from jax.sharding import PartitionSpec as P

RB = 64


def shift(value, axis, step):
    count = lax.axis_size(axis)
    return lax.ppermute(value, axis, [(i, (i + step) % count) for i in range(count)])


def shards(
    slopes_in, basis_left, basis_right, rank_blocks, tile_owner, footprint, trace_weight, fitting
):
    frames = slopes_in.shape[0]
    rows_here, slots_here, tile_size, rank_cols = basis_left.shape
    columns, rows, dirs = lax.axis_size("col"), lax.axis_size("row"), lax.axis_size("dir")
    col, row, direction = lax.axis_index("col"), lax.axis_index("row"), lax.axis_index("dir")
    group = rows * dirs
    mine = row * dirs + direction
    piece = frames // (columns * group)
    width = slots_here * tile_size
    points = rows_here * tile_size

    pieces = slopes_in.reshape(columns, group, piece, width)
    held = []
    for s in range(columns):
        part = lax.dynamic_index_in_dim(pieces, (col + s) % columns, 0, keepdims=False)
        part = lax.dynamic_index_in_dim(part, mine, 0, keepdims=False)
        held.append(part if s == 0 else shift(part, "col", s))
    blocks = jnp.stack(held).reshape(columns, piece, slots_here, tile_size)
    blocks = blocks.transpose(0, 2, 1, 3).reshape(columns * slots_here, piece, tile_size)
    owner_col, owner_slot = tile_owner // slots_here, tile_owner % slots_here
    place = ((col - owner_col) % columns) * slots_here + owner_slot
    got = []
    for s in range(columns):
        want = lax.dynamic_slice_in_dim(place, ((col + s) % columns) * slots_here, slots_here, 0)
        part = jnp.take(blocks, want, axis=0)
        got.append(part if s == 0 else shift(part, "col", s))
    chosen = jnp.stack(got, axis=1)
    chosen = jnp.stack([chosen] + [shift(chosen, "row", -t) for t in range(1, rows)], axis=2)
    chosen = jnp.stack([chosen] + [shift(chosen, "dir", -t) for t in range(1, dirs)], axis=3)
    chosen = chosen.reshape(slots_here, frames, tile_size)

    live = jnp.arange(rank_cols, dtype=jnp.int32) // RB < rank_blocks[:, :, None]
    coeffs = jnp.einsum("kfn,iknr->ikfr", chosen, basis_right, preferred_element_type=jnp.float32)
    coeffs = jnp.where(live[:, :, None, :], coeffs, 0.0).astype(jnp.bfloat16)
    summed = jnp.einsum("ikfr,iknr->fin", coeffs, basis_left, preferred_element_type=jnp.float32)
    summed = summed.astype(jnp.bfloat16).reshape(columns, frames // columns, points)
    total = summed[0].astype(jnp.float32)
    for s in range(1, columns):
        total = total + shift(summed[s], "col", -s).astype(jnp.float32)
    layer_block = total.astype(jnp.bfloat16)

    layer_count, taps, pupil_count = footprint.shape[1:]
    per_layer = points * group // layer_count
    shifts = (jnp.arange(layer_count, dtype=jnp.int32) * per_layer)[:, None, None]
    flat = (footprint[0] + shifts).reshape(layer_count * taps, pupil_count)
    weight = trace_weight[0].reshape(layer_count * taps, pupil_count)
    if per_layer % points == 0:
        near = True
    else:
        near = False

    def tap_matrix(dr, dd):
        q = ((row + dr) % rows) * dirs + (direction + dd) % dirs
        f, w = flat, weight
        if near:
            first = (q * points // per_layer) * taps
            f = lax.dynamic_slice_in_dim(flat, first, taps, 0)
            w = lax.dynamic_slice_in_dim(weight, first, taps, 0)
        here = q * points + jnp.arange(points, dtype=jnp.int32)
        out = jnp.zeros((points, pupil_count), jnp.float32)
        for c in range(f.shape[0]):
            out = out + jnp.where(here[:, None] == f[c][None, :], w[c][None, :], 0.0)
        return out.astype(jnp.bfloat16)

    matrix = [[tap_matrix(dr, dd) for dd in range(dirs)] for dr in range(rows)]

    share = frames // columns
    order = layer_block.reshape(rows, dirs, piece, points)
    result = []
    for s in range(columns):
        here = order if s == 0 else shift(order, "col", s)
        pupil = jnp.zeros((share, pupil_count), jnp.float32)
        for dr in range(rows):
            far = here if dr == 0 else jnp.roll(shift(here, "row", -dr), dr, axis=0)
            for dd in range(dirs):
                block = far if dd == 0 else jnp.roll(shift(far, "dir", -dd), dd, axis=1)
                pupil = pupil + jnp.dot(
                    block.reshape(share, points),
                    matrix[dr][dd],
                    preferred_element_type=jnp.float32,
                )
        pupil = pupil.astype(jnp.bfloat16)
        result.append(
            jnp.dot(pupil, fitting, preferred_element_type=jnp.float32).astype(jnp.bfloat16)
        )
    commands = jnp.stack(result).reshape(columns, rows, dirs, piece, -1)
    commands = jnp.take(commands, (col - jnp.arange(columns)) % columns, axis=0)
    commands = jnp.take(commands, (jnp.arange(rows) - row) % rows, axis=1)
    commands = jnp.take(commands, (jnp.arange(dirs) - direction) % dirs, axis=2)
    return commands.reshape(1, frames, -1)


def solution(mesh):
    placed = (
        P(None, ("grp", "col")),
        P(("row", "dir"), "col", None, None),
        P(("row", "dir"), "col", None, None),
        P(("row", "dir"), "col"),
        P(),
        P(("row", "dir"), None, None, None),
        P(("row", "dir"), None, None, None),
        P(None, "col"),
    )
    return jax.shard_map(
        shards,
        mesh=mesh,
        in_specs=placed,
        out_specs=P(("row", "dir"), "grp", "col"),
        check_vma=False,
    )
```

```python
import functools

import jax
import jax.numpy as jnp
from jax import lax
from jax.experimental import pallas as pl
from jax.experimental.pallas import tpu as pltpu
from jax.sharding import PartitionSpec as P

RB = 64


def shift(value, axis, step):
    count = lax.axis_size(axis)
    return lax.ppermute(value, axis, [(i, (i + step) % count) for i in range(count)])


def wide(
    slopes_in, basis_left, basis_right, rank_blocks, tile_owner, footprint, trace_weight, fitting
):
    frames = slopes_in.shape[0]
    rows_here, slots_here, tile_size, rank_cols = basis_left.shape
    columns, rows, dirs = lax.axis_size("col"), lax.axis_size("row"), lax.axis_size("dir")
    col, row, direction = lax.axis_index("col"), lax.axis_index("row"), lax.axis_index("dir")
    group = rows * dirs
    mine = row * dirs + direction
    piece = frames // (columns * group)
    width = slots_here * tile_size
    points = rows_here * tile_size

    pieces = slopes_in.reshape(columns, group, piece, width)
    held = []
    for s in range(columns):
        part = lax.dynamic_index_in_dim(pieces, (col + s) % columns, 0, keepdims=False)
        part = lax.dynamic_index_in_dim(part, mine, 0, keepdims=False)
        held.append(part if s == 0 else shift(part, "col", s))
    blocks = jnp.stack(held).reshape(columns, piece, slots_here, tile_size)
    blocks = blocks.transpose(0, 2, 1, 3).reshape(columns * slots_here, piece, tile_size)
    owner_col, owner_slot = tile_owner // slots_here, tile_owner % slots_here
    place = ((col - owner_col) % columns) * slots_here + owner_slot
    got = []
    for s in range(columns):
        want = lax.dynamic_slice_in_dim(place, ((col + s) % columns) * slots_here, slots_here, 0)
        part = jnp.take(blocks, want, axis=0)
        got.append(part if s == 0 else shift(part, "col", s))
    chosen = jnp.stack(got, axis=1)
    chosen = jnp.stack([chosen] + [shift(chosen, "row", -t) for t in range(1, rows)], axis=2)
    chosen = jnp.stack([chosen] + [shift(chosen, "dir", -t) for t in range(1, dirs)], axis=3)
    chosen = chosen.reshape(slots_here, frames, tile_size)

    live = jnp.arange(rank_cols, dtype=jnp.int32) // RB < rank_blocks[:, :, None]
    coeffs = jnp.einsum("kfn,iknr->ikfr", chosen, basis_right, preferred_element_type=jnp.float32)
    coeffs = jnp.where(live[:, :, None, :], coeffs, 0.0).astype(jnp.bfloat16)
    summed = jnp.einsum("ikfr,iknr->fin", coeffs, basis_left, preferred_element_type=jnp.float32)
    summed = summed.astype(jnp.bfloat16).reshape(columns, frames // columns, points)
    total = summed[0].astype(jnp.float32)
    for s in range(1, columns):
        total = total + shift(summed[s], "col", -s).astype(jnp.float32)
    layer_block = total.astype(jnp.bfloat16)

    layer_count, taps, pupil_count = footprint.shape[1:]
    per_layer = points * group // layer_count
    shifts = (jnp.arange(layer_count, dtype=jnp.int32) * per_layer)[:, None, None]
    flat = (footprint[0] + shifts).reshape(layer_count * taps, pupil_count)
    weight = trace_weight[0].reshape(layer_count * taps, pupil_count)
    if per_layer % points == 0:
        near = True
    else:
        near = False

    def tap_matrix(dr, dd):
        q = ((row + dr) % rows) * dirs + (direction + dd) % dirs
        f, w = flat, weight
        if near:
            first = (q * points // per_layer) * taps
            f = lax.dynamic_slice_in_dim(flat, first, taps, 0)
            w = lax.dynamic_slice_in_dim(weight, first, taps, 0)
        here = q * points + jnp.arange(points, dtype=jnp.int32)
        out = jnp.zeros((points, pupil_count), jnp.float32)
        for c in range(f.shape[0]):
            out = out + jnp.where(here[:, None] == f[c][None, :], w[c][None, :], 0.0)
        return out.astype(jnp.bfloat16)

    matrix = [[tap_matrix(dr, dd) for dd in range(dirs)] for dr in range(rows)]

    share = frames // columns
    order = layer_block.reshape(rows, dirs, piece, points)
    result = []
    for s in range(columns):
        here = order if s == 0 else shift(order, "col", s)
        pupil = jnp.zeros((share, pupil_count), jnp.float32)
        for dr in range(rows):
            far = here if dr == 0 else jnp.roll(shift(here, "row", -dr), dr, axis=0)
            for dd in range(dirs):
                block = far if dd == 0 else jnp.roll(shift(far, "dir", -dd), dd, axis=1)
                pupil = pupil + jnp.dot(
                    block.reshape(share, points),
                    matrix[dr][dd],
                    preferred_element_type=jnp.float32,
                )
        pupil = pupil.astype(jnp.bfloat16)
        result.append(
            jnp.dot(pupil, fitting, preferred_element_type=jnp.float32).astype(jnp.bfloat16)
        )
    commands = jnp.stack(result).reshape(columns, rows, dirs, piece, -1)
    commands = jnp.take(commands, (col - jnp.arange(columns)) % columns, axis=0)
    commands = jnp.take(commands, (jnp.arange(rows) - row) % rows, axis=1)
    commands = jnp.take(commands, (jnp.arange(dirs) - direction) % dirs, axis=2)
    return commands.reshape(1, frames, -1)


WHOLE = pl.BlockSpec(memory_space=pltpu.VMEM)
SCALARS = pl.BlockSpec(memory_space=pltpu.SMEM)


def tap_kernel(per_layer, dr, dd, place_ref, foot_ref, weight_ref, out_ref):
    points, pupil_count = out_ref.shape
    taps = foot_ref.shape[1]
    first = ((place_ref[1] ^ dr) * 2 + (place_ref[2] ^ dd)) * points
    layer = first // per_layer
    base = first - layer * per_layer
    wide = 256
    tall = 16

    def lanes(j, _):
        cols = pl.ds(pl.multiple_of(j * wide, wide), wide)
        foot = [
            jnp.broadcast_to(foot_ref[layer, c : c + 1, cols] - base, (tall, wide))
            for c in range(taps)
        ]
        weight = [
            jnp.broadcast_to(weight_ref[layer, c : c + 1, cols], (tall, wide)) for c in range(taps)
        ]
        spot = lax.broadcasted_iota(jnp.int32, (tall, wide), 0)

        def slab(i, _):
            here = spot + i * tall
            total = jnp.where(here == foot[0], weight[0], 0.0)
            for c in range(1, taps):
                total = total + jnp.where(here == foot[c], weight[c], 0.0)
            out_ref[pl.ds(pl.multiple_of(i * tall, tall), tall), cols] = total.astype(jnp.bfloat16)
            return 0

        lax.fori_loop(0, points // tall, slab, 0, unroll=4)
        return 0

    lax.fori_loop(0, pupil_count // wide, lanes, 0)


def tap_matrix(place, footprint, weight, dr, dd, points, per_layer):
    pupil_count = footprint.shape[2]
    taps = footprint.shape[1]
    return pl.pallas_call(
        functools.partial(tap_kernel, per_layer, dr, dd),
        out_shape=jax.ShapeDtypeStruct((points, pupil_count), jnp.bfloat16),
        in_specs=[SCALARS, WHOLE, WHOLE],
        out_specs=WHOLE,
        cost_estimate=pl.CostEstimate(
            flops=400 * points * pupil_count,
            bytes_accessed=2 * points * pupil_count,
            transcendentals=0,
        ),
        compiler_params=pltpu.CompilerParams(vmem_limit_bytes=8 << 20),
        name="tap_matrix",
    )(place, footprint, weight)


def pick_kernel(place_ref, owner_ref, *refs):
    columns = (len(refs) - 1) // 2
    held_refs, got_refs, held = refs[:columns], refs[columns:-1], refs[-1]
    piece, width = held_refs[0].shape
    slots_here = owner_ref.shape[0] // columns
    tile_size = width // slots_here
    col = place_ref[0]
    for s in range(columns):
        held[s] = held_refs[s][...]
    for s in range(columns):
        for j in range(slots_here):
            block = owner_ref[(col ^ s) * slots_here + j]
            source = col ^ (block // slots_here)
            lane = pl.multiple_of((block % slots_here) * tile_size, tile_size)
            got_refs[s][:, j * tile_size : (j + 1) * tile_size] = held[
                source, :, pl.ds(lane, tile_size)
            ]


def pick_blocks(place, tile_owner, held):
    columns = len(held)
    return pl.pallas_call(
        pick_kernel,
        out_shape=[jax.ShapeDtypeStruct(held[0].shape, held[0].dtype)] * columns,
        in_specs=[SCALARS, SCALARS] + [WHOLE] * columns,
        out_specs=[WHOLE] * columns,
        scratch_shapes=[pltpu.VMEM((columns,) + held[0].shape, held[0].dtype)],
        cost_estimate=pl.CostEstimate(flops=1 << 20, bytes_accessed=1 << 19, transcendentals=0),
        compiler_params=pltpu.CompilerParams(vmem_limit_bytes=4 << 20),
        name="pick_blocks",
    )(place, tile_owner, *held)


def partial_kernel(place_ref, rank_ref, own_ref, other_ref, right_ref, left_ref, *refs):
    out_refs, all_ref = refs[:-1], refs[-1]
    rows_here, slots_here, tile_size, rank_cols = left_ref.shape
    columns, piece, width = own_ref.shape
    here = place_ref[2]
    rows = 2 * columns * piece
    column = lax.broadcasted_iota(jnp.int32, (rows, rank_cols), 1) // RB
    for which, ref in enumerate((own_ref, other_ref)):
        spot = here if which == 0 else 1 - here
        for s in range(columns):
            first = pl.multiple_of((2 * s + spot) * piece, piece)
            all_ref[pl.ds(first, piece), :] = ref[s]
    for i in range(rows_here):
        total = None
        for k in range(slots_here):
            coeffs = jnp.dot(
                all_ref[:, k * tile_size : (k + 1) * tile_size],
                right_ref[i, k],
                preferred_element_type=jnp.float32,
            )
            coeffs = jnp.where(column < rank_ref[i, k], coeffs, 0.0).astype(jnp.bfloat16)
            term = lax.dot_general(
                coeffs,
                left_ref[i, k],
                (((1,), (1,)), ((), ())),
                preferred_element_type=jnp.float32,
            )
            total = term if total is None else total + term
        total = total.astype(jnp.bfloat16)
        for s in range(columns):
            out_refs[s][:, i * tile_size : (i + 1) * tile_size] = total[
                2 * s * piece : 2 * (s + 1) * piece
            ]


def partial_sums(place, ranks, own, other, right, left):
    rows_here, slots_here, tile_size, rank_cols = left.shape
    columns, piece, width = own.shape
    out = jax.ShapeDtypeStruct((2 * piece, rows_here * tile_size), jnp.bfloat16)
    return pl.pallas_call(
        partial_kernel,
        out_shape=[out] * columns,
        in_specs=[SCALARS, SCALARS] + [WHOLE] * 4,
        out_specs=[WHOLE] * columns,
        scratch_shapes=[pltpu.VMEM((2 * columns * piece, width), jnp.bfloat16)],
        cost_estimate=pl.CostEstimate(
            flops=8 * columns * piece * rows_here * slots_here * tile_size * rank_cols,
            bytes_accessed=4 * right.size,
            transcendentals=0,
        ),
        compiler_params=pltpu.CompilerParams(vmem_limit_bytes=12 << 20),
        name="partial_sums",
    )(place, ranks, own, other, right, left)


def command_kernel(count, wide, last, *refs):
    refs = list(refs)
    place_ref = refs.pop(0) if last else None
    fields = [[refs.pop(0) for _ in range(4)] for _ in range(count)]
    matrix = [refs.pop(0) for _ in range(4)]
    fit_ref = refs.pop(0)
    early = [refs.pop(0) for _ in range(last)]
    out_ref, field_ref, pupil_ref = refs
    share, points = fields[0][0].shape
    half = share // 2
    for n, parts in enumerate(fields):
        for j, ref in enumerate(parts):
            cols = slice(j * points, (j + 1) * points)
            if j % 2 == 0:
                field_ref[n * share : (n + 1) * share, cols] = ref[...]
            else:
                field_ref[n * share : n * share + half, cols] = ref[half:]
                field_ref[n * share + half : (n + 1) * share, cols] = ref[:half]

    for j in range(pupil_ref.shape[1] // wide):
        cols = slice(j * wide, (j + 1) * wide)
        total = None
        for c in range(4):
            term = jnp.dot(
                field_ref[:, c * points : (c + 1) * points],
                matrix[c][:, cols],
                preferred_element_type=jnp.float32,
            )
            total = term if total is None else total + term
        pupil_ref[:, cols] = total.astype(jnp.bfloat16)

    def put(done, cols, value):
        for h in range(2):
            spot = (place_ref[0] ^ done) * 2 + (place_ref[1] ^ h)
            spot = pl.multiple_of(spot * half, half)
            out_ref[pl.ds(spot, half), cols] = value[h * half : (h + 1) * half]

    before = 0
    for ref in early:
        for n in range(ref.shape[0] // share):
            put(before, slice(None), ref[n * share : (n + 1) * share])
            before += 1
    for j in range(fit_ref.shape[1] // wide):
        cols = slice(j * wide, (j + 1) * wide)
        value = jnp.dot(
            pupil_ref[...], fit_ref[:, cols], preferred_element_type=jnp.float32
        ).astype(jnp.bfloat16)
        if last:
            for n in range(count):
                put(before + n, cols, value[n * share : (n + 1) * share])
        else:
            out_ref[:, cols] = value


def command_rows(fields, matrix, fitting, early=(), place=None, frames=0):
    count = len(fields)
    share, points = fields[0][0].shape
    pupil_count, acts = fitting.shape
    last = len(early)
    rows = frames if last else count * share
    flat = [part for parts in fields for part in parts]
    operands = ([place] if last else []) + flat + list(matrix) + [fitting] + list(early)
    specs = ([SCALARS] if last else []) + [WHOLE] * (len(operands) - (1 if last else 0))
    return pl.pallas_call(
        functools.partial(command_kernel, count, 256, last),
        out_shape=jax.ShapeDtypeStruct((rows, acts), jnp.bfloat16),
        in_specs=specs,
        out_specs=WHOLE,
        scratch_shapes=[
            pltpu.VMEM((count * share, 4 * points), jnp.bfloat16),
            pltpu.VMEM((count * share, pupil_count), jnp.bfloat16),
        ],
        cost_estimate=pl.CostEstimate(
            flops=2 * count * share * pupil_count * (4 * points + acts),
            bytes_accessed=4 * rows * acts,
            transcendentals=0,
        ),
        compiler_params=pltpu.CompilerParams(vmem_limit_bytes=26 << 20),
        name="command_rows",
    )(*operands)


def swap(value, axis, step):
    return lax.ppermute(value, axis, [(i, i ^ step) for i in range(lax.axis_size(axis))])


def after(values, *others):
    flat, tree = jax.tree.flatten((values, others))
    return jax.tree.unflatten(tree, lax.optimization_barrier(flat))


def narrow(
    slopes_in, basis_left, basis_right, rank_blocks, tile_owner, footprint, trace_weight, fitting
):
    frames = slopes_in.shape[0]
    rows_here, slots_here, tile_size, rank_cols = basis_left.shape
    columns, rows, dirs = lax.axis_size("col"), lax.axis_size("row"), lax.axis_size("dir")
    col, row, direction = lax.axis_index("col"), lax.axis_index("row"), lax.axis_index("dir")
    place = jnp.stack([col, row, direction]).astype(jnp.int32)
    group = rows * dirs
    mine = row * dirs + direction
    piece = frames // (columns * group)
    points = rows_here * tile_size
    per_layer = points * group // footprint.shape[1]

    def taps(dr, dd):
        return tap_matrix(place, footprint[0], trace_weight[0], dr, dd, points, per_layer)

    matrix = [taps(0, 0), taps(1, 0), taps(0, 1), taps(1, 1)]

    held = []
    for s in range(columns):
        spot = ((col ^ s) * group + mine) * piece
        part = lax.dynamic_slice_in_dim(slopes_in, spot, piece, 0)
        held.append(part if s == 0 else swap(part, "col", s))
    held, (matrix[0],) = after(held, matrix[0])
    got = pick_blocks(place, tile_owner, held)
    got = [got[s] if s == 0 else swap(got[s], "col", s) for s in range(columns)]
    got, (matrix[1],) = after(got, matrix[1])
    own = jnp.stack(got)
    over = swap(own, "row", 1)
    sibling = swap(own, "dir", 1)
    near_sums = partial_sums(place, rank_blocks, own, sibling, basis_right, basis_left)
    near_in = [near_sums[0]] + [swap(near_sums[s], "col", s) for s in range(1, columns)]
    over, (near_sums, matrix[2]) = after(over, near_sums, matrix[2])
    far = swap(over, "dir", 1)
    far_sums = partial_sums(place, rank_blocks, over, far, basis_right, basis_left)
    far_in = [far_sums[0]] + [swap(far_sums[s], "col", s) for s in range(1, columns)]

    def add(parts):
        total = parts[0].astype(jnp.float32)
        for part in parts[1:]:
            total = total + part.astype(jnp.float32)
        return total.astype(jnp.bfloat16)

    near_in, (matrix[3],) = after(near_in, matrix[3])
    layers = jnp.concatenate([add(near_in), add(far_in)], axis=0)

    fields = []
    for s in range(columns):
        here = layers if s == 0 else swap(layers, "col", s)
        over = swap(here, "row", 1)
        fields.append([here, over, swap(here, "dir", 1), swap(over, "dir", 1)])
    early = [command_rows(fields[:2], matrix, fitting)]
    for s in range(2, columns - 1):
        early.append(command_rows(fields[s : s + 1], matrix, fitting))
    commands = command_rows(fields[columns - 1 :], matrix, fitting, early, place, frames)
    return commands[None]


def shards(*args):
    frames = args[0].shape[0]
    points = args[1].shape[0] * args[1].shape[2]
    columns, rows, dirs = lax.axis_size("col"), lax.axis_size("row"), lax.axis_size("dir")
    per_layer = points * rows * dirs // args[5].shape[1]
    piece = frames // (columns * rows * dirs)
    fits = piece % 16 == 0 and per_layer % points == 0
    if rows == 2 and dirs == 2 and columns > 2 and columns & (columns - 1) == 0 and fits:
        return narrow(*args)
    return wide(*args)


def solution(mesh):
    placed = (
        P(None, ("grp", "col")),
        P(("row", "dir"), "col", None, None),
        P(("row", "dir"), "col", None, None),
        P(("row", "dir"), "col"),
        P(),
        P(("row", "dir"), None, None, None),
        P(("row", "dir"), None, None, None),
        P(None, "col"),
    )
    return jax.shard_map(
        shards,
        mesh=mesh,
        in_specs=placed,
        out_specs=P(("row", "dir"), "grp", "col"),
        check_vma=False,
    )
```

```python
import functools

import jax
import jax.numpy as jnp
from jax import lax
from jax.experimental import pallas as pl
from jax.experimental.pallas import tpu as pltpu
from jax.sharding import PartitionSpec as P


RB = 64


def shift(value, axis, step):
    count = lax.axis_size(axis)
    return lax.ppermute(value, axis, [(i, (i + step) % count) for i in range(count)])


def wide(
    slopes_in, basis_left, basis_right, rank_blocks, tile_owner, footprint, trace_weight, fitting
):
    frames = slopes_in.shape[0]
    rows_here, slots_here, tile_size, rank_cols = basis_left.shape
    columns, rows, dirs = lax.axis_size("col"), lax.axis_size("row"), lax.axis_size("dir")
    col, row, direction = lax.axis_index("col"), lax.axis_index("row"), lax.axis_index("dir")
    group = rows * dirs
    mine = row * dirs + direction
    piece = frames // (columns * group)
    width = slots_here * tile_size
    points = rows_here * tile_size

    pieces = slopes_in.reshape(columns, group, piece, width)
    held = []
    for s in range(columns):
        part = lax.dynamic_index_in_dim(pieces, (col + s) % columns, 0, keepdims=False)
        part = lax.dynamic_index_in_dim(part, mine, 0, keepdims=False)
        held.append(part if s == 0 else shift(part, "col", s))
    blocks = jnp.stack(held).reshape(columns, piece, slots_here, tile_size)
    blocks = blocks.transpose(0, 2, 1, 3).reshape(columns * slots_here, piece, tile_size)
    owner_col, owner_slot = tile_owner // slots_here, tile_owner % slots_here
    place = ((col - owner_col) % columns) * slots_here + owner_slot
    got = []
    for s in range(columns):
        want = lax.dynamic_slice_in_dim(place, ((col + s) % columns) * slots_here, slots_here, 0)
        part = jnp.take(blocks, want, axis=0)
        got.append(part if s == 0 else shift(part, "col", s))
    chosen = jnp.stack(got, axis=1)
    chosen = jnp.stack([chosen] + [shift(chosen, "row", -t) for t in range(1, rows)], axis=2)
    chosen = jnp.stack([chosen] + [shift(chosen, "dir", -t) for t in range(1, dirs)], axis=3)
    chosen = chosen.reshape(slots_here, frames, tile_size)

    live = jnp.arange(rank_cols, dtype=jnp.int32) // RB < rank_blocks[:, :, None]
    coeffs = jnp.einsum("kfn,iknr->ikfr", chosen, basis_right, preferred_element_type=jnp.float32)
    coeffs = jnp.where(live[:, :, None, :], coeffs, 0.0).astype(jnp.bfloat16)
    summed = jnp.einsum("ikfr,iknr->fin", coeffs, basis_left, preferred_element_type=jnp.float32)
    summed = summed.astype(jnp.bfloat16).reshape(columns, frames // columns, points)
    total = summed[0].astype(jnp.float32)
    for s in range(1, columns):
        total = total + shift(summed[s], "col", -s).astype(jnp.float32)
    layer_block = total.astype(jnp.bfloat16)

    layer_count, taps, pupil_count = footprint.shape[1:]
    per_layer = points * group // layer_count
    shifts = (jnp.arange(layer_count, dtype=jnp.int32) * per_layer)[:, None, None]
    flat = (footprint[0] + shifts).reshape(layer_count * taps, pupil_count)
    weight = trace_weight[0].reshape(layer_count * taps, pupil_count)
    if per_layer % points == 0:
        near = True
    else:
        near = False

    def tap_matrix(dr, dd):
        q = ((row + dr) % rows) * dirs + (direction + dd) % dirs
        f, w = flat, weight
        if near:
            first = (q * points // per_layer) * taps
            f = lax.dynamic_slice_in_dim(flat, first, taps, 0)
            w = lax.dynamic_slice_in_dim(weight, first, taps, 0)
        here = q * points + jnp.arange(points, dtype=jnp.int32)
        out = jnp.zeros((points, pupil_count), jnp.float32)
        for c in range(f.shape[0]):
            out = out + jnp.where(here[:, None] == f[c][None, :], w[c][None, :], 0.0)
        return out.astype(jnp.bfloat16)

    matrix = [[tap_matrix(dr, dd) for dd in range(dirs)] for dr in range(rows)]

    share = frames // columns
    order = layer_block.reshape(rows, dirs, piece, points)
    result = []
    for s in range(columns):
        here = order if s == 0 else shift(order, "col", s)
        pupil = jnp.zeros((share, pupil_count), jnp.float32)
        for dr in range(rows):
            far = here if dr == 0 else jnp.roll(shift(here, "row", -dr), dr, axis=0)
            for dd in range(dirs):
                block = far if dd == 0 else jnp.roll(shift(far, "dir", -dd), dd, axis=1)
                pupil = pupil + jnp.dot(
                    block.reshape(share, points),
                    matrix[dr][dd],
                    preferred_element_type=jnp.float32,
                )
        pupil = pupil.astype(jnp.bfloat16)
        result.append(
            jnp.dot(pupil, fitting, preferred_element_type=jnp.float32).astype(jnp.bfloat16)
        )
    commands = jnp.stack(result).reshape(columns, rows, dirs, piece, -1)
    commands = jnp.take(commands, (col - jnp.arange(columns)) % columns, axis=0)
    commands = jnp.take(commands, (jnp.arange(rows) - row) % rows, axis=1)
    commands = jnp.take(commands, (jnp.arange(dirs) - direction) % dirs, axis=2)
    return commands.reshape(1, frames, -1)


WHOLE = pl.BlockSpec(memory_space=pltpu.VMEM)
SCALARS = pl.BlockSpec(memory_space=pltpu.SMEM)


def tap_kernel(per_layer, dr, dd, foot_ref, weight_ref, out_ref):
    points, pupil_count = out_ref.shape
    taps = foot_ref.shape[1]
    first = ((lax.axis_index("row") ^ dr) * 2 + (lax.axis_index("dir") ^ dd)) * points
    layer = first // per_layer
    base = first - layer * per_layer
    wide = 256
    tall = 16
    block = 256

    def lanes(j, _):
        cols = pl.ds(pl.multiple_of(j * wide, wide), wide)
        weight = [
            jnp.broadcast_to(
                weight_ref[layer, c : c + 1, cols].astype(jnp.bfloat16), (tall, wide)
            )
            for c in range(taps)
        ]
        spot = lax.broadcasted_iota(jnp.int32, (tall, wide), 0)
        spot = spot.astype(jnp.float32).astype(jnp.bfloat16)
        zero = jnp.zeros((tall, wide), jnp.bfloat16)
        for b in range(points // block):
            foot = []
            for c in range(taps):
                near = foot_ref[layer, c : c + 1, cols] - (base + b * block)
                near = jnp.where((near >= 0) & (near < block), near, -1)
                near = near.astype(jnp.float32).astype(jnp.bfloat16)
                foot.append(jnp.broadcast_to(near, (tall, wide)))
            for i in range(block // tall):
                here = spot + jnp.bfloat16(i * tall)
                total = jnp.where(here == foot[0], weight[0], zero)
                for c in range(1, taps):
                    total = total + jnp.where(here == foot[c], weight[c], zero)
                first = b * block + i * tall
                out_ref[first : first + tall, cols] = total
        return 0

    lax.fori_loop(0, pupil_count // wide, lanes, 0)


def tap_matrix(footprint, weight, dr, dd, points, per_layer):
    pupil_count = footprint.shape[2]
    return pl.pallas_call(
        functools.partial(tap_kernel, per_layer, dr, dd),
        out_shape=jax.ShapeDtypeStruct((points, pupil_count), jnp.bfloat16),
        in_specs=[WHOLE, WHOLE],
        out_specs=WHOLE,
        cost_estimate=pl.CostEstimate(
            flops=400 * points * pupil_count,
            bytes_accessed=2 * points * pupil_count,
            transcendentals=0,
        ),
        compiler_params=pltpu.CompilerParams(vmem_limit_bytes=8 << 20),
        name="tap_matrix",
    )(footprint, weight)


def pick_kernel(blocks, place_ref, *refs):
    columns = (len(refs) - 1) // 2
    held_refs, got_refs, held = refs[:columns], refs[columns:-1], refs[-1]
    _, width = held_refs[0].shape
    slots_here = blocks // columns
    tile_size = width // slots_here
    col = place_ref[0]
    for s in range(columns):
        held[s] = held_refs[s][...]
    for s in range(columns):
        for j in range(slots_here):
            block = place_ref[3 + (col ^ s) * slots_here + j]
            source = col ^ (block // slots_here)
            lane = pl.multiple_of((block % slots_here) * tile_size, tile_size)
            got_refs[s][:, j * tile_size : (j + 1) * tile_size] = held[
                source, :, pl.ds(lane, tile_size)
            ]


def pick_blocks(place, blocks, held):
    columns = len(held)
    return pl.pallas_call(
        functools.partial(pick_kernel, blocks),
        out_shape=[jax.ShapeDtypeStruct(held[0].shape, held[0].dtype)] * columns,
        in_specs=[SCALARS] + [WHOLE] * columns,
        out_specs=[WHOLE] * columns,
        scratch_shapes=[pltpu.VMEM((columns,) + held[0].shape, held[0].dtype)],
        cost_estimate=pl.CostEstimate(flops=1 << 20, bytes_accessed=1 << 19, transcendentals=0),
        compiler_params=pltpu.CompilerParams(vmem_limit_bytes=4 << 20),
        name="pick_blocks",
    )(place, *held)


def partial_kernel(place_ref, own_ref, other_ref, right_ref, left_ref, *refs):
    out_refs, all_ref = refs[:-1], refs[-1]
    rows_here, slots_here, tile_size, rank_cols = left_ref.shape
    columns, piece, _ = own_ref.shape
    here = place_ref[2]
    rows = 2 * columns * piece
    ranks = 3 + columns * slots_here
    column = lax.broadcasted_iota(jnp.int32, (rows, rank_cols), 1) // RB
    for which, ref in enumerate((own_ref, other_ref)):
        spot = here if which == 0 else 1 - here
        for s in range(columns):
            first = pl.multiple_of((2 * s + spot) * piece, piece)
            all_ref[pl.ds(first, piece), :] = ref[s]
    for i in range(rows_here):
        total = None
        for k in range(slots_here):
            coeffs = jnp.dot(
                all_ref[:, k * tile_size : (k + 1) * tile_size],
                right_ref[i, k],
                preferred_element_type=jnp.float32,
            )
            coeffs = jnp.where(column < place_ref[ranks + i * slots_here + k], coeffs, 0.0).astype(jnp.bfloat16)
            term = lax.dot_general(
                coeffs,
                left_ref[i, k],
                (((1,), (1,)), ((), ())),
                preferred_element_type=jnp.float32,
            )
            total = term if total is None else total + term
        total = total.astype(jnp.bfloat16)
        for s in range(columns):
            out_refs[s][:, i * tile_size : (i + 1) * tile_size] = total[
                2 * s * piece : 2 * (s + 1) * piece
            ]


def partial_sums(place, own, other, right, left):
    rows_here, slots_here, tile_size, rank_cols = left.shape
    columns, piece, width = own.shape
    out = jax.ShapeDtypeStruct((2 * piece, rows_here * tile_size), jnp.bfloat16)
    return pl.pallas_call(
        partial_kernel,
        out_shape=[out] * columns,
        in_specs=[SCALARS] + [WHOLE] * 4,
        out_specs=[WHOLE] * columns,
        scratch_shapes=[pltpu.VMEM((2 * columns * piece, width), jnp.bfloat16)],
        cost_estimate=pl.CostEstimate(
            flops=8 * columns * piece * rows_here * slots_here * tile_size * rank_cols,
            bytes_accessed=4 * right.size,
            transcendentals=0,
        ),
        compiler_params=pltpu.CompilerParams(vmem_limit_bytes=12 << 20),
        name="partial_sums",
    )(place, own, other, right, left)


def command_kernel(wide, shares, *refs):
    refs = list(refs)
    parts = [refs.pop(0) for _ in range(4)]
    matrix = [refs.pop(0) for _ in range(4)]
    fit_ref = refs.pop(0)
    early = len(shares) - 1
    done = [refs.pop(0) for _ in range(early)]
    out_ref, field_ref, pupil_ref = refs[:3]
    share, points = parts[0].shape
    half = share // 2
    sent = []

    def send(source, s, h, cols):
        spot = (lax.axis_index("col") ^ s) * 2 + (lax.axis_index("row") ^ h)
        spot = pl.multiple_of(spot * half, half)
        copy = pltpu.make_async_copy(
            source.at[h * half : (h + 1) * half, cols],
            out_ref.at[pl.ds(spot, half), cols],
            refs[4].at[len(sent)],
        )
        copy.start()
        sent.append(copy)

    for s, ref in zip(shares, done):
        for h in range(2):
            send(ref, s, h, slice(None))
    for j, ref in enumerate(parts):
        cols = slice(j * points, (j + 1) * points)
        if j % 2 == 0:
            field_ref[:, cols] = ref[...]
        else:
            field_ref[:half, cols] = ref[half:]
            field_ref[half:, cols] = ref[:half]

    for j in range(pupil_ref.shape[1] // wide):
        cols = slice(j * wide, (j + 1) * wide)
        total = None
        for c in range(4):
            term = jnp.dot(
                field_ref[:, c * points : (c + 1) * points],
                matrix[c][:, cols],
                preferred_element_type=jnp.float32,
            )
            total = term if total is None else total + term
        pupil_ref[:, cols] = total.astype(jnp.bfloat16)

    value_ref = refs[3] if early else out_ref
    for j in range(fit_ref.shape[1] // wide):
        cols = slice(j * wide, (j + 1) * wide)
        value_ref[:, cols] = jnp.dot(
            pupil_ref[...], fit_ref[:, cols], preferred_element_type=jnp.float32
        ).astype(jnp.bfloat16)
        for h in range(2 if early else 0):
            send(value_ref, shares[-1], h, cols)
    for copy in sent:
        copy.wait()


def command_rows(parts, matrix, fitting, early=(), shares=(0,), frames=0):
    share, points = parts[0].shape
    pupil_count, acts = fitting.shape
    wide = 256
    operands = list(parts) + list(matrix) + [fitting] + list(early)
    scratch = [
        pltpu.VMEM((share, 4 * points), jnp.bfloat16),
        pltpu.VMEM((share, pupil_count), jnp.bfloat16),
    ]
    if early:
        scratch.append(pltpu.VMEM((share, acts), jnp.bfloat16))
        scratch.append(pltpu.SemaphoreType.DMA((2 * len(early) + 2 * (acts // wide),)))
    return pl.pallas_call(
        functools.partial(command_kernel, wide, shares),
        out_shape=jax.ShapeDtypeStruct((frames if early else share, acts), jnp.bfloat16),
        in_specs=[WHOLE] * len(operands),
        out_specs=pl.BlockSpec(memory_space=pltpu.HBM) if early else WHOLE,
        scratch_shapes=scratch,
        cost_estimate=pl.CostEstimate(
            flops=2 * share * pupil_count * (4 * points + acts),
            bytes_accessed=4 * share * acts,
            transcendentals=0,
        ),
        compiler_params=pltpu.CompilerParams(vmem_limit_bytes=26 << 20),
        name="command_rows",
    )(*operands)


def pass_kernel(own_ref, other_ref, out_ref):
    col = lax.axis_index("col")
    outer = (col == 0) | (col == lax.axis_size("col") - 1)

    @pl.when(outer)
    def _():
        out_ref[...] = own_ref[...]

    @pl.when(jnp.logical_not(outer))
    def _():
        out_ref[...] = other_ref[...]


def pass_on(own, other):
    return pl.pallas_call(
        pass_kernel,
        out_shape=jax.ShapeDtypeStruct(own.shape, own.dtype),
        in_specs=[WHOLE, WHOLE],
        out_specs=WHOLE,
        cost_estimate=pl.CostEstimate(flops=1 << 18, bytes_accessed=1 << 19, transcendentals=0),
        compiler_params=pltpu.CompilerParams(vmem_limit_bytes=2 << 20),
        name="pass_on",
    )(own, other)


def swap(value, axis, step):
    return lax.ppermute(value, axis, [(i, i ^ step) for i in range(lax.axis_size(axis))])


def after(values, *others):
    flat, tree = jax.tree.flatten((values, others))
    return jax.tree.unflatten(tree, lax.optimization_barrier(flat))


def narrow(
    slopes_in, basis_left, basis_right, rank_blocks, tile_owner, footprint, trace_weight, fitting
):
    frames = slopes_in.shape[0]
    rows_here, _, tile_size, _ = basis_left.shape
    columns, rows, dirs = lax.axis_size("col"), lax.axis_size("row"), lax.axis_size("dir")
    col, row, direction = lax.axis_index("col"), lax.axis_index("row"), lax.axis_index("dir")
    place = jnp.stack([col, row, direction]).astype(jnp.int32)
    place = jnp.concatenate([place, tile_owner, rank_blocks.reshape(-1)])
    group = rows * dirs
    mine = row * dirs + direction
    piece = frames // (columns * group)
    points = rows_here * tile_size
    per_layer = points * group // footprint.shape[1]

    def taps(dr, dd):
        return tap_matrix(footprint[0], trace_weight[0], dr, dd, points, per_layer)

    matrix = [taps(0, 0), taps(1, 0), taps(0, 1), taps(1, 1)]

    def exchange(parts):
        return [parts[0]] + [swap(parts[s], "col", s) for s in range(1, columns)]

    held = []
    for s in range(columns):
        spot = ((col ^ s) * group + mine) * piece
        held.append(lax.dynamic_slice_in_dim(slopes_in, spot, piece, 0))
    held = exchange(held)
    held, (matrix[0],) = after(held, matrix[0])
    got = exchange(pick_blocks(place, tile_owner.shape[0], held))
    got, (matrix[1],) = after(got, matrix[1])
    own = jnp.stack(got)
    over = swap(own, "row", 1)
    sibling = swap(own, "dir", 1)
    near_sums = partial_sums(place, own, sibling, basis_right, basis_left)
    near_in = exchange(near_sums)
    far_sums = partial_sums(place, over, swap(over, "dir", 1), basis_right, basis_left)
    far_in = exchange(far_sums)

    def add(parts):
        total = parts[0].astype(jnp.float32)
        for part in parts[1:]:
            total = total + part.astype(jnp.float32)
        return total.astype(jnp.bfloat16)

    near_in, _ = after(near_in, far_sums)
    layers = [jnp.concatenate([add(near_in), add(far_in)], axis=0)] * columns
    layers[3] = swap(layers[0], "col", 3)
    layers[1] = swap(layers[0], "col", 1)
    onward = pass_on(layers[0], layers[3])
    layers[2] = lax.ppermute(onward, "col", [(0, 2), (1, 0), (2, 3), (3, 1)])

    early = []
    shares = (0, 3, 1, 2)
    for s in shares:
        here = layers[s]
        over = swap(here, "row", 1)
        field = [here, over, swap(here, "dir", 1), swap(over, "dir", 1)]
        if s != shares[-1]:
            early.append(command_rows(field, matrix, fitting))
        else:
            commands = command_rows(field, matrix, fitting, early, shares, frames)
    return commands[None]


def shards(*args):
    frames = args[0].shape[0]
    points = args[1].shape[0] * args[1].shape[2]
    columns, rows, dirs = lax.axis_size("col"), lax.axis_size("row"), lax.axis_size("dir")
    per_layer = points * rows * dirs // args[5].shape[1]
    piece = frames // (columns * rows * dirs)
    fits = piece % 16 == 0 and per_layer % points == 0 and points % 256 == 0
    if rows == 2 and dirs == 2 and columns == 4 and fits:
        return narrow(*args)
    return wide(*args)


def solution(mesh):
    placed = (
        P(None, ("grp", "col")),
        P(("row", "dir"), "col", None, None),
        P(("row", "dir"), "col", None, None),
        P(("row", "dir"), "col"),
        P(),
        P(("row", "dir"), None, None, None),
        P(("row", "dir"), None, None, None),
        P(None, "col"),
    )
    return jax.shard_map(
        shards,
        mesh=mesh,
        in_specs=placed,
        out_specs=P(("row", "dir"), "grp", "col"),
        check_vma=False,
    )
```

```python
import functools

import jax
import jax.numpy as jnp
from jax import lax
from jax.experimental import pallas as pl
from jax.experimental.pallas import tpu as pltpu
from jax.sharding import PartitionSpec as P


RB = 64


def shift(value, axis, step):
    count = lax.axis_size(axis)
    return lax.ppermute(value, axis, [(i, (i + step) % count) for i in range(count)])


def wide(
    slopes_in, basis_left, basis_right, rank_blocks, tile_owner, footprint, trace_weight, fitting
):
    frames = slopes_in.shape[0]
    rows_here, slots_here, tile_size, rank_cols = basis_left.shape
    columns, rows, dirs = lax.axis_size("col"), lax.axis_size("row"), lax.axis_size("dir")
    col, row, direction = lax.axis_index("col"), lax.axis_index("row"), lax.axis_index("dir")
    group = rows * dirs
    mine = row * dirs + direction
    piece = frames // (columns * group)
    width = slots_here * tile_size
    points = rows_here * tile_size

    pieces = slopes_in.reshape(columns, group, piece, width)
    held = []
    for s in range(columns):
        part = lax.dynamic_index_in_dim(pieces, (col + s) % columns, 0, keepdims=False)
        part = lax.dynamic_index_in_dim(part, mine, 0, keepdims=False)
        held.append(part if s == 0 else shift(part, "col", s))
    blocks = jnp.stack(held).reshape(columns, piece, slots_here, tile_size)
    blocks = blocks.transpose(0, 2, 1, 3).reshape(columns * slots_here, piece, tile_size)
    owner_col, owner_slot = tile_owner // slots_here, tile_owner % slots_here
    place = ((col - owner_col) % columns) * slots_here + owner_slot
    got = []
    for s in range(columns):
        want = lax.dynamic_slice_in_dim(place, ((col + s) % columns) * slots_here, slots_here, 0)
        part = jnp.take(blocks, want, axis=0)
        got.append(part if s == 0 else shift(part, "col", s))
    chosen = jnp.stack(got, axis=1)
    chosen = jnp.stack([chosen] + [shift(chosen, "row", -t) for t in range(1, rows)], axis=2)
    chosen = jnp.stack([chosen] + [shift(chosen, "dir", -t) for t in range(1, dirs)], axis=3)
    chosen = chosen.reshape(slots_here, frames, tile_size)

    live = jnp.arange(rank_cols, dtype=jnp.int32) // RB < rank_blocks[:, :, None]
    coeffs = jnp.einsum("kfn,iknr->ikfr", chosen, basis_right, preferred_element_type=jnp.float32)
    coeffs = jnp.where(live[:, :, None, :], coeffs, 0.0).astype(jnp.bfloat16)
    summed = jnp.einsum("ikfr,iknr->fin", coeffs, basis_left, preferred_element_type=jnp.float32)
    summed = summed.astype(jnp.bfloat16).reshape(columns, frames // columns, points)
    total = summed[0].astype(jnp.float32)
    for s in range(1, columns):
        total = total + shift(summed[s], "col", -s).astype(jnp.float32)
    layer_block = total.astype(jnp.bfloat16)

    layer_count, taps, pupil_count = footprint.shape[1:]
    per_layer = points * group // layer_count
    shifts = (jnp.arange(layer_count, dtype=jnp.int32) * per_layer)[:, None, None]
    flat = (footprint[0] + shifts).reshape(layer_count * taps, pupil_count)
    weight = trace_weight[0].reshape(layer_count * taps, pupil_count)
    if per_layer % points == 0:
        near = True
    else:
        near = False

    def tap_matrix(dr, dd):
        q = ((row + dr) % rows) * dirs + (direction + dd) % dirs
        f, w = flat, weight
        if near:
            first = (q * points // per_layer) * taps
            f = lax.dynamic_slice_in_dim(flat, first, taps, 0)
            w = lax.dynamic_slice_in_dim(weight, first, taps, 0)
        here = q * points + jnp.arange(points, dtype=jnp.int32)
        out = jnp.zeros((points, pupil_count), jnp.float32)
        for c in range(f.shape[0]):
            out = out + jnp.where(here[:, None] == f[c][None, :], w[c][None, :], 0.0)
        return out.astype(jnp.bfloat16)

    matrix = [[tap_matrix(dr, dd) for dd in range(dirs)] for dr in range(rows)]

    share = frames // columns
    order = layer_block.reshape(rows, dirs, piece, points)
    result = []
    for s in range(columns):
        here = order if s == 0 else shift(order, "col", s)
        pupil = jnp.zeros((share, pupil_count), jnp.float32)
        for dr in range(rows):
            far = here if dr == 0 else jnp.roll(shift(here, "row", -dr), dr, axis=0)
            for dd in range(dirs):
                block = far if dd == 0 else jnp.roll(shift(far, "dir", -dd), dd, axis=1)
                pupil = pupil + jnp.dot(
                    block.reshape(share, points),
                    matrix[dr][dd],
                    preferred_element_type=jnp.float32,
                )
        pupil = pupil.astype(jnp.bfloat16)
        result.append(
            jnp.dot(pupil, fitting, preferred_element_type=jnp.float32).astype(jnp.bfloat16)
        )
    commands = jnp.stack(result).reshape(columns, rows, dirs, piece, -1)
    commands = jnp.take(commands, (col - jnp.arange(columns)) % columns, axis=0)
    commands = jnp.take(commands, (jnp.arange(rows) - row) % rows, axis=1)
    commands = jnp.take(commands, (jnp.arange(dirs) - direction) % dirs, axis=2)
    return commands.reshape(1, frames, -1)


WHOLE = pl.BlockSpec(memory_space=pltpu.VMEM)
SCALARS = pl.BlockSpec(memory_space=pltpu.SMEM)


def tap_kernel(per_layer, dr, dd, foot_ref, weight_ref, out_ref):
    points, pupil_count = out_ref.shape
    taps = foot_ref.shape[1]
    first = ((lax.axis_index("row") ^ dr) * 2 + (lax.axis_index("dir") ^ dd)) * points
    layer = first // per_layer
    base = first - layer * per_layer
    wide = 256
    tall = 16
    block = 256

    def lanes(j, _):
        cols = pl.ds(pl.multiple_of(j * wide, wide), wide)
        weight = [
            jnp.broadcast_to(
                weight_ref[layer, c : c + 1, cols].astype(jnp.bfloat16), (tall, wide)
            )
            for c in range(taps)
        ]
        spot = lax.broadcasted_iota(jnp.int32, (tall, wide), 0)
        spot = spot.astype(jnp.float32).astype(jnp.bfloat16)
        zero = jnp.zeros((tall, wide), jnp.bfloat16)
        for b in range(points // block):
            foot = []
            for c in range(taps):
                near = foot_ref[layer, c : c + 1, cols] - (base + b * block)
                near = jnp.where((near >= 0) & (near < block), near, -1)
                near = near.astype(jnp.float32).astype(jnp.bfloat16)
                foot.append(jnp.broadcast_to(near, (tall, wide)))
            for i in range(block // tall):
                here = spot + jnp.bfloat16(i * tall)
                total = jnp.where(here == foot[0], weight[0], zero)
                for c in range(1, taps):
                    total = total + jnp.where(here == foot[c], weight[c], zero)
                first = b * block + i * tall
                out_ref[first : first + tall, cols] = total
        return 0

    lax.fori_loop(0, pupil_count // wide, lanes, 0)


def tap_matrix(footprint, weight, dr, dd, points, per_layer):
    pupil_count = footprint.shape[2]
    return pl.pallas_call(
        functools.partial(tap_kernel, per_layer, dr, dd),
        out_shape=jax.ShapeDtypeStruct((points, pupil_count), jnp.bfloat16),
        in_specs=[WHOLE, WHOLE],
        out_specs=WHOLE,
        cost_estimate=pl.CostEstimate(
            flops=400 * points * pupil_count,
            bytes_accessed=2 * points * pupil_count,
            transcendentals=0,
        ),
        compiler_params=pltpu.CompilerParams(vmem_limit_bytes=8 << 20),
        name="tap_matrix",
    )(footprint, weight)


def pick_kernel(blocks, place_ref, *refs):
    columns = (len(refs) - 1) // 2
    held_refs, got_refs, held = refs[:columns], refs[columns:-1], refs[-1]
    _, width = held_refs[0].shape
    slots_here = blocks // columns
    tile_size = width // slots_here
    col = place_ref[0]
    for s in range(columns):
        held[s] = held_refs[s][...]
    for s in range(columns):
        for j in range(slots_here):
            block = place_ref[3 + (col ^ s) * slots_here + j]
            source = col ^ (block // slots_here)
            lane = pl.multiple_of((block % slots_here) * tile_size, tile_size)
            got_refs[s][:, j * tile_size : (j + 1) * tile_size] = held[
                source, :, pl.ds(lane, tile_size)
            ]


def pick_blocks(place, blocks, held):
    columns = len(held)
    return pl.pallas_call(
        functools.partial(pick_kernel, blocks),
        out_shape=[jax.ShapeDtypeStruct(held[0].shape, held[0].dtype)] * columns,
        in_specs=[SCALARS] + [WHOLE] * columns,
        out_specs=[WHOLE] * columns,
        scratch_shapes=[pltpu.VMEM((columns,) + held[0].shape, held[0].dtype)],
        cost_estimate=pl.CostEstimate(flops=1 << 20, bytes_accessed=1 << 19, transcendentals=0),
        compiler_params=pltpu.CompilerParams(vmem_limit_bytes=4 << 20),
        name="pick_blocks",
    )(place, *held)


def partial_kernel(place_ref, own_ref, other_ref, right_ref, left_ref, *refs):
    out_refs, all_ref = refs[:-1], refs[-1]
    rows_here, slots_here, tile_size, rank_cols = left_ref.shape
    columns, piece, _ = own_ref.shape
    here = place_ref[2]
    rows = 2 * columns * piece
    ranks = 3 + columns * slots_here
    column = lax.broadcasted_iota(jnp.int32, (rows, rank_cols), 1) // RB
    for which, ref in enumerate((own_ref, other_ref)):
        spot = here if which == 0 else 1 - here
        for s in range(columns):
            first = pl.multiple_of((2 * s + spot) * piece, piece)
            all_ref[pl.ds(first, piece), :] = ref[s]
    for i in range(rows_here):
        total = None
        for k in range(slots_here):
            coeffs = jnp.dot(
                all_ref[:, k * tile_size : (k + 1) * tile_size],
                right_ref[i, k],
                preferred_element_type=jnp.float32,
            )
            coeffs = jnp.where(column < place_ref[ranks + i * slots_here + k], coeffs, 0.0).astype(jnp.bfloat16)
            term = lax.dot_general(
                coeffs,
                left_ref[i, k],
                (((1,), (1,)), ((), ())),
                preferred_element_type=jnp.float32,
            )
            total = term if total is None else total + term
        total = total.astype(jnp.bfloat16)
        for s in range(columns):
            out_refs[s][:, i * tile_size : (i + 1) * tile_size] = total[
                2 * s * piece : 2 * (s + 1) * piece
            ]


def partial_sums(place, own, other, right, left):
    rows_here, slots_here, tile_size, rank_cols = left.shape
    columns, piece, width = own.shape
    out = jax.ShapeDtypeStruct((2 * piece, rows_here * tile_size), jnp.bfloat16)
    return pl.pallas_call(
        partial_kernel,
        out_shape=[out] * columns,
        in_specs=[SCALARS] + [WHOLE] * 4,
        out_specs=[WHOLE] * columns,
        scratch_shapes=[pltpu.VMEM((2 * columns * piece, width), jnp.bfloat16)],
        cost_estimate=pl.CostEstimate(
            flops=8 * columns * piece * rows_here * slots_here * tile_size * rank_cols,
            bytes_accessed=4 * right.size,
            transcendentals=0,
        ),
        compiler_params=pltpu.CompilerParams(vmem_limit_bytes=12 << 20),
        name="partial_sums",
    )(place, own, other, right, left)


def half_kernel(wide, own_ref, same_ref, first_ref, second_ref, out_ref):
    for j in range(out_ref.shape[1] // wide):
        cols = slice(j * wide, (j + 1) * wide)
        out_ref[:, cols] = jnp.dot(
            own_ref[...], first_ref[:, cols], preferred_element_type=jnp.float32
        ) + jnp.dot(same_ref[...], second_ref[:, cols], preferred_element_type=jnp.float32)


def half_pupil(own, same, first, second):
    share, points = own.shape
    pupil_count = first.shape[1]
    return pl.pallas_call(
        functools.partial(half_kernel, 256),
        out_shape=jax.ShapeDtypeStruct((share, pupil_count), jnp.float32),
        in_specs=[WHOLE] * 4,
        out_specs=WHOLE,
        cost_estimate=pl.CostEstimate(
            flops=4 * share * points * pupil_count,
            bytes_accessed=4 * share * pupil_count,
            transcendentals=0,
        ),
        compiler_params=pltpu.CompilerParams(vmem_limit_bytes=8 << 20),
        name="half_pupil",
    )(own, same, first, second)


def command_kernel(wide, shares, chunks, *refs):
    refs = list(refs)
    parts = [refs.pop(0) for _ in chunks]
    matrix = [refs.pop(0) for _ in chunks]
    fit_ref = refs.pop(0)
    base_ref = refs.pop(0) if len(chunks) < 4 else None
    early = len(shares) - 1
    done = [refs.pop(0) for _ in range(early)]
    out_ref, field_ref, pupil_ref = refs[:3]
    share, points = parts[0].shape
    half = share // 2
    sent = []

    def send(source, s, h, cols):
        spot = (lax.axis_index("col") ^ s) * 2 + (lax.axis_index("row") ^ h)
        spot = pl.multiple_of(spot * half, half)
        copy = pltpu.make_async_copy(
            source.at[h * half : (h + 1) * half, cols],
            out_ref.at[pl.ds(spot, half), cols],
            refs[4].at[len(sent)],
        )
        copy.start()
        sent.append(copy)

    for s, ref in zip(shares, done):
        for h in range(2):
            send(ref, s, h, slice(None))
    for j, ref in enumerate(parts):
        cols = slice(j * points, (j + 1) * points)
        if chunks[j] % 2 == 0:
            field_ref[:, cols] = ref[...]
        else:
            field_ref[:half, cols] = ref[half:]
            field_ref[half:, cols] = ref[:half]

    for j in range(pupil_ref.shape[1] // wide):
        cols = slice(j * wide, (j + 1) * wide)
        total = None if base_ref is None else base_ref[:, cols]
        for c in range(len(chunks)):
            term = jnp.dot(
                field_ref[:, c * points : (c + 1) * points],
                matrix[c][:, cols],
                preferred_element_type=jnp.float32,
            )
            total = term if total is None else total + term
        pupil_ref[:, cols] = total.astype(jnp.bfloat16)

    value_ref = refs[3] if early else out_ref
    for j in range(fit_ref.shape[1] // wide):
        cols = slice(j * wide, (j + 1) * wide)
        value_ref[:, cols] = jnp.dot(
            pupil_ref[...], fit_ref[:, cols], preferred_element_type=jnp.float32
        ).astype(jnp.bfloat16)
        for h in range(2 if early else 0):
            send(value_ref, shares[-1], h, cols)
    for copy in sent:
        copy.wait()


def command_rows(parts, matrix, fitting, early=(), shares=(0,), frames=0, base=None):
    share, points = parts[0].shape
    pupil_count, acts = fitting.shape
    wide = 256
    chunks = tuple(range(4)) if base is None else (1, 3)
    operands = [parts[c] for c in chunks] + [matrix[c] for c in chunks] + [fitting]
    operands += ([] if base is None else [base]) + list(early)
    scratch = [
        pltpu.VMEM((share, len(chunks) * points), jnp.bfloat16),
        pltpu.VMEM((share, pupil_count), jnp.bfloat16),
    ]
    if early:
        scratch.append(pltpu.VMEM((share, acts), jnp.bfloat16))
        scratch.append(pltpu.SemaphoreType.DMA((2 * len(early) + 2 * (acts // wide),)))
    return pl.pallas_call(
        functools.partial(command_kernel, wide, shares, chunks),
        out_shape=jax.ShapeDtypeStruct((frames if early else share, acts), jnp.bfloat16),
        in_specs=[WHOLE] * len(operands),
        out_specs=pl.BlockSpec(memory_space=pltpu.HBM) if early else WHOLE,
        scratch_shapes=scratch,
        cost_estimate=pl.CostEstimate(
            flops=2 * share * pupil_count * (4 * points + acts),
            bytes_accessed=4 * share * acts,
            transcendentals=0,
        ),
        compiler_params=pltpu.CompilerParams(vmem_limit_bytes=26 << 20),
        name="command_rows",
    )(*operands)


def pass_kernel(own_ref, other_ref, out_ref):
    col = lax.axis_index("col")
    outer = (col == 0) | (col == lax.axis_size("col") - 1)

    @pl.when(outer)
    def _():
        out_ref[...] = own_ref[...]

    @pl.when(jnp.logical_not(outer))
    def _():
        out_ref[...] = other_ref[...]


def pass_on(own, other):
    return pl.pallas_call(
        pass_kernel,
        out_shape=jax.ShapeDtypeStruct(own.shape, own.dtype),
        in_specs=[WHOLE, WHOLE],
        out_specs=WHOLE,
        cost_estimate=pl.CostEstimate(flops=1 << 18, bytes_accessed=1 << 19, transcendentals=0),
        compiler_params=pltpu.CompilerParams(vmem_limit_bytes=2 << 20),
        name="pass_on",
    )(own, other)


def swap(value, axis, step):
    return lax.ppermute(value, axis, [(i, i ^ step) for i in range(lax.axis_size(axis))])


def after(values, *others):
    flat, tree = jax.tree.flatten((values, others))
    return jax.tree.unflatten(tree, lax.optimization_barrier(flat))


def narrow(
    slopes_in, basis_left, basis_right, rank_blocks, tile_owner, footprint, trace_weight, fitting
):
    frames = slopes_in.shape[0]
    rows_here, _, tile_size, _ = basis_left.shape
    columns, rows, dirs = lax.axis_size("col"), lax.axis_size("row"), lax.axis_size("dir")
    col, row, direction = lax.axis_index("col"), lax.axis_index("row"), lax.axis_index("dir")
    place = jnp.stack([col, row, direction]).astype(jnp.int32)
    place = jnp.concatenate([place, tile_owner, rank_blocks.reshape(-1)])
    group = rows * dirs
    mine = row * dirs + direction
    piece = frames // (columns * group)
    points = rows_here * tile_size
    per_layer = points * group // footprint.shape[1]

    def taps(dr, dd):
        return tap_matrix(footprint[0], trace_weight[0], dr, dd, points, per_layer)

    matrix = [taps(0, 0), taps(1, 0), taps(0, 1), taps(1, 1)]

    def exchange(parts):
        return [parts[0]] + [swap(parts[s], "col", s) for s in range(1, columns)]

    held = []
    for s in range(columns):
        spot = ((col ^ s) * group + mine) * piece
        held.append(lax.dynamic_slice_in_dim(slopes_in, spot, piece, 0))
    held = exchange(held)
    held, (matrix[0],) = after(held, matrix[0])
    got = exchange(pick_blocks(place, tile_owner.shape[0], held))
    got, (matrix[1],) = after(got, matrix[1])
    own = jnp.stack(got)
    over = swap(own, "row", 1)
    sibling = swap(own, "dir", 1)
    near_sums = partial_sums(place, own, sibling, basis_right, basis_left)
    near_in = exchange(near_sums)
    far_sums = partial_sums(place, over, swap(over, "dir", 1), basis_right, basis_left)
    far_in = exchange(far_sums)

    def add(parts):
        total = parts[0].astype(jnp.float32)
        for part in parts[1:]:
            total = total + part.astype(jnp.float32)
        return total.astype(jnp.bfloat16)

    near_in, _ = after(near_in, far_sums)
    layers = [jnp.concatenate([add(near_in), add(far_in)], axis=0)] * columns
    layers[3] = swap(layers[0], "col", 3)
    layers[1] = swap(layers[0], "col", 1)
    onward = pass_on(layers[0], layers[3])
    layers[2] = lax.ppermute(onward, "col", [(0, 2), (1, 0), (2, 3), (3, 1)])

    early = []
    shares = (0, 3, 1, 2)
    for s in shares:
        here = layers[s]
        over = swap(here, "row", 1)
        field = [here, over, swap(here, "dir", 1), swap(over, "dir", 1)]
        if s != shares[-1]:
            early.append(command_rows(field, matrix, fitting))
        else:
            base = half_pupil(field[0], field[2], matrix[0], matrix[2])
            commands = command_rows(field, matrix, fitting, early, shares, frames, base)
    return commands[None]


def shards(*args):
    frames = args[0].shape[0]
    points = args[1].shape[0] * args[1].shape[2]
    columns, rows, dirs = lax.axis_size("col"), lax.axis_size("row"), lax.axis_size("dir")
    per_layer = points * rows * dirs // args[5].shape[1]
    piece = frames // (columns * rows * dirs)
    fits = piece % 16 == 0 and per_layer % points == 0 and points % 256 == 0
    if rows == 2 and dirs == 2 and columns == 4 and fits:
        return narrow(*args)
    return wide(*args)


def solution(mesh):
    placed = (
        P(None, ("grp", "col")),
        P(("row", "dir"), "col", None, None),
        P(("row", "dir"), "col", None, None),
        P(("row", "dir"), "col"),
        P(),
        P(("row", "dir"), None, None, None),
        P(("row", "dir"), None, None, None),
        P(None, "col"),
    )
    return jax.shard_map(
        shards,
        mesh=mesh,
        in_specs=placed,
        out_specs=P(("row", "dir"), "grp", "col"),
        check_vma=False,
    )
```
